32 devices in a mesh: tm: 8 (over z, x), space: 4 (over y, core).
Axes of the slice: x: 2, y: 2, z: 4, core: 2. Of those that a mesh axis runs over, the one named last changes fastest.
Arguments:
- state: float32 [32, 16, 64, 128], P('tm', 'space'), may hold values from -6 to 6
- source: float32 [32, 16, 64, 128], P('tm', 'space'), may hold values from -6 to 6
- absorption: float32 [16, 64, 128], P('space'), may hold values from 0.05 to 0.5
Outputs:
- relaxed: float32 [32, 16, 64, 128], P('tm', 'space')
- coarse_residual: float32 [8, 16, 64, 128], P('tm', 'space')
- residual_norm: float32 [], replicated
The draws below stay inside these ranges and needn't reach their ends.
All inputs are finite; a program needn't handle non-finite values.
Results may differ from the reference program's by a relative error of at most 0.0004.
Values sent between devices are 32-bit elements; how exact they have to be, the bound alone decides.
A program may use at most 64 MiB of HBM per device.

```python
import math
import jax
import jax.numpy as jnp

NX = 64
NY = 128
CF = 4
SWEEPS = 5
NC = 8
NT = 32
NZ = 16


def shard_levels(stream_key, dims, cuts, low, high):
    level, own = 1.0, jax.random.fold_in(stream_key, 6)
    for dim, shards_of in cuts:
        steps = jnp.exp(jax.random.uniform(jax.random.fold_in(own, dim), (shards_of,), jnp.float32, low / len(cuts), high / len(cuts)))
        level = level * jnp.repeat(steps, dims[dim] // shards_of).reshape([-1 if axis == dim else 1 for axis in range(len(dims))])
    return level


def scatter_about(key, dims, deviation, limit, split=(), kind=jnp.bfloat16):
    drawn = deviation * jax.random.normal(key, dims, jnp.float32)
    if split:
        drawn = drawn * shard_levels(key, dims, split, -0.22, 0.18)
    return jnp.clip(drawn, -limit, limit).astype(kind)


def setup_inputs(seed: int = 0) -> dict:
    arg_keys = jax.random.split(jax.random.key(seed), 4)
    return {
        "state": scatter_about(arg_keys[0], (NT, NZ, NX, NY), 1.0, 6.0, ((0, 8), (1, 4)), jnp.float32),
        "source": scatter_about(arg_keys[1], (NT, NZ, NX, NY), 1.0, 6.0, ((0, 8), (1, 4)), jnp.float32),
        "absorption": jnp.clip(jnp.exp(math.log(0.5) - 2.3025851 * jax.random.uniform(arg_keys[2], (NZ, NX, NY), jnp.float32) ** shard_levels(arg_keys[2], (NZ, NX, NY), ((0, 4),), -0.2, 0.2)), 0.05, 0.5),
    }


coupling = 4.0


def sweep_weights(count):
    spread = 6.0 * coupling / (1.0 + 6.0 * coupling)
    return [1.0 / (1.0 + spread * math.cos(math.pi * (2 * k + 1) / (2 * count))) for k in range(count)]


def apply_operator(field, diag):
    lead = [(0, 0)] * (field.ndim - 3)
    padded = jnp.pad(field, lead + [(1, 1), (1, 1), (1, 1)])
    beside = padded[..., 2:, 1:-1, 1:-1] + padded[..., :-2, 1:-1, 1:-1]
    beside = beside + padded[..., 1:-1, 2:, 1:-1] + padded[..., 1:-1, :-2, 1:-1]
    beside = beside + padded[..., 1:-1, 1:-1, 2:] + padded[..., 1:-1, 1:-1, :-2]
    return diag * field - coupling * beside


def implicit_step(rhs, diag):
    field = rhs / diag
    for weight in sweep_weights(SWEEPS):
        field = field + weight * (rhs - apply_operator(field, diag)) / diag
    return field


def reference(state, source, absorption):
    diag = 1.0 + 6.0 * coupling + absorption
    fine = state.reshape(NC, CF, NZ, NX, NY)
    rhs = source.reshape(NC, CF, NZ, NX, NY)
    points = [fine[:, j] for j in range(CF)]

    def relax_fine(points):
        for j in range(1, CF):
            points[j] = implicit_step(points[j - 1], diag) + rhs[:, j]
        return points

    def previous(last):
        return jnp.concatenate([jnp.zeros_like(last[:1]), last[:-1]], axis=0)

    points = relax_fine(points)
    points[0] = implicit_step(previous(points[-1]), diag) + rhs[:, 0]
    points = relax_fine(points)
    coarse_residual = rhs[:, 0] + implicit_step(previous(points[-1]), diag) - points[0]
    relaxed = jnp.stack(points, axis=1).reshape(NT, NZ, NX, NY)
    return relaxed, coarse_residual, jnp.sum(coarse_residual * coarse_residual)
```

```python
import functools
import math

import jax
import jax.numpy as jnp
import numpy as np
from jax import lax
from jax.experimental import pallas as pl
from jax.experimental.pallas import tpu as pltpu
from jax.sharding import PartitionSpec as P

CF = 4
SWEEPS = 5
SUB = 8

coupling = 4.0
MESH = pl.DeviceIdType.MESH


def series():
    spread = 6.0 * coupling / (1.0 + 6.0 * coupling)
    one = np.polynomial.Polynomial([1.0])
    var = np.polynomial.Polynomial([0.0, 1.0])
    x = one
    for k in range(SWEEPS):
        weight = 1.0 / (1.0 + spread * math.cos(math.pi * (2 * k + 1) / (2 * SWEEPS)))
        x = x + weight * (one - (one - var) * x)
    c = x.coef
    return float(c[0]), float(c[2]), float(c[4])


def kernel(nt, ns, state, source, absorb, relaxed, resid, norm,
           nat, c4, work, held, full, pfull, qown, qin, tot, allsp, alltm, parts,
           loc_sem, g_send, g_recv, p_send, p_recv, sh_send, q_send, q_recv,
           n_send, n_recv):
    tm = lax.axis_index("tm")
    s = lax.axis_index("space")
    depth, rows, cols = absorb.shape
    lo = rows // SUB
    layers = ns * depth
    others = ns // 2 - 1
    partner = s + 1 - 2 * lax.rem(s, 2)
    chips = [lax.rem(s + 2 * i, ns) for i in range(1, others + 1)]
    r0, r1, r2 = series()
    own = s * depth

    barrier = pltpu.get_barrier_semaphore()
    for i in range(1, ns):
        pl.semaphore_signal(barrier, inc=1, device_id=(tm, lax.rem(s + i, ns)), device_id_type=MESH)
    for i in range(1, nt):
        pl.semaphore_signal(barrier, inc=1, device_id=(lax.rem(tm + i, nt), s), device_id_type=MESH)

    srcs = [absorb, state.at[0]] + [source.at[j] for j in range(1, CF)] + [source.at[0]]
    fields = len(srcs)
    quarter = lambda f, q: nat.at[f, pl.ds(q * depth, depth)]
    loads = [pltpu.make_async_copy(srcs[f], quarter(f, s), loc_sem.at[f]) for f in range(fields)]
    for load in loads:
        load.start()
    work[0] = jnp.zeros(work.shape[1:], jnp.float32)
    work[layers + 1] = jnp.zeros(work.shape[1:], jnp.float32)

    pl.semaphore_wait(barrier, ns - 1 + nt - 1)

    def remote(src, dst, send, recv, where):
        return pltpu.make_async_remote_copy(
            src_ref=src, dst_ref=dst, send_sem=send, recv_sem=recv,
            device_id=where, device_id_type=MESH)

    pending = []

    def go(copy):
        copy.start()
        pending.append(copy)

    for f in range(fields):
        for i, chip in enumerate(chips):
            go(remote(srcs[f], quarter(f, s), g_send.at[f, 1 + i], g_recv.at[f, s], (tm, chip)))
        go(remote(srcs[f], quarter(f, s), g_send.at[f, 0], g_recv.at[f, s], (tm, partner)))

    def relay(f):
        for i, chip in enumerate(chips):
            here = quarter(f, chip)
            remote(here, here, g_send.at[f, 0], g_recv.at[f, chip], (tm, partner)).wait_recv()
            go(remote(here, here, g_send.at[f, 1 + others + i], g_recv.at[f, chip], (tm, partner)))

    def arrive(f, mine=True):
        if mine:
            loads[f].wait()
        there = [partner] + [lax.rem(partner + 2 * i, ns) for i in range(1, others + 1)]
        for q in there:
            here = quarter(f, q)
            remote(here, here, g_send.at[f, 0], g_recv.at[f, q], (tm, partner)).wait_recv()

    def natural(f, z):
        return jnp.stack([nat[f, z, pl.ds(i, SUB, stride=lo), :] for i in range(lo)])

    lane = lax.broadcasted_iota(jnp.int32, (lo, SUB, cols), 2)
    first_lane, last_lane = lane == 0, lane == cols - 1
    sub = lax.broadcasted_iota(jnp.int32, (SUB, cols), 0)
    first_sub, last_sub = sub == 0, sub == SUB - 1

    def beside(v):
        up = jnp.where(first_sub, 0.0, pltpu.roll(v[lo - 1], 1, 0))
        down = jnp.where(last_sub, 0.0, pltpu.roll(v[0], SUB - 1, 0))
        total = jnp.concatenate([up[None], v[:-1]]) + jnp.concatenate([v[1:], down[None]])
        flat = v.reshape(lo * SUB, cols)
        left = pltpu.roll(flat, 1, 1).reshape(v.shape)
        right = pltpu.roll(flat, cols - 1, 1).reshape(v.shape)
        return total + jnp.where(first_lane, 0.0, left) + jnp.where(last_lane, 0.0, right)

    def sweep(finish, unroll=4):
        def body(i, carry):
            before, now = carry
            for j in range(unroll):
                z = i * unroll + j
                after = work[z + 2]
                finish(z, c4[z] * (before + after + beside(now)), now)
                before, now = now, after
            return before, now
        lax.fori_loop(0, layers // unroll, body, (work[0], work[1]))

    def plain(z, moved, now):
        work[z + 1] = moved

    def adding(factor):
        def finish(z, moved, now):
            work[z + 1] = moved + factor * held[z]
        return finish

    def start_with(z, value):
        h = value * (c4[z] * (r2 / coupling))
        work[z + 1] = h
        held[z] = h

    def phi(finish):
        sweep(plain)
        sweep(adding(r1 / r2))
        sweep(plain)
        sweep(adding(r0 / r2))
        sweep(finish)

    def each_layer(do):
        def body(z, _):
            do(z)
            return 0
        lax.fori_loop(0, layers, body, 0)

    def onward(f):
        def finish(z, moved, now):
            value = now + moved + natural(f, z)
            full[z] = value
            start_with(z, value)
        return finish

    def to_full(z, moved, now):
        full[z] = now + moved

    def put(ref, d, value):
        for i in range(lo):
            ref[d, pl.ds(i, SUB, stride=lo), :] = value[i]

    relay(0)
    relay(1)
    arrive(0)

    def scale(z):
        c4[z] = coupling / (1.0 + 6.0 * coupling + natural(0, z))
    each_layer(scale)
    relay(2)
    arrive(1)
    each_layer(lambda z: start_with(z, natural(1, z)))
    relay(3)
    arrive(2)
    phi(onward(2))
    relay(4)
    arrive(3)
    phi(onward(3))
    phi(to_full)
    relay(5)

    loads[4].wait()
    chunk = lambda d: pl.ds(own + d, 1)
    for d in range(depth):
        qown[0, d] = full[own + d] + natural(4, own + d)
    shifts = [remote(qown.at[0, pl.ds(d, 1)], pfull.at[chunk(d)], sh_send.at[d], p_recv.at[d, s],
                     (lax.rem(tm + 1, nt), s)) for d in range(depth)]

    @pl.when(tm < nt - 1)
    def _():
        for shift in shifts:
            shift.start()

    @pl.when(tm == 0)
    def _():
        def zero(z):
            pfull[z] = jnp.zeros(pfull.shape[1:], jnp.float32)
        each_layer(zero)

    @pl.when(tm > 0)
    def _():
        copies = []

        def send(src, send_sem, recv_sem, where):
            copy = remote(src, src, send_sem, recv_sem, where)
            copy.start()
            copies.append(copy)

        for d in range(depth):
            here = pfull.at[chunk(d)]
            shifts[d].wait_recv()
            for i, chip in enumerate(chips):
                send(here, p_send.at[d, 1 + i], p_recv.at[d, s], (tm, chip))
            send(here, p_send.at[d, 0], p_recv.at[d, s], (tm, partner))
        for d in range(depth):
            for i, chip in enumerate(chips):
                here = pfull.at[pl.ds(chip * depth + d, 1)]
                remote(here, here, p_send.at[d, 0], p_recv.at[d, chip], (tm, partner)).wait_recv()
                send(here, p_send.at[d, 1 + others + i], p_recv.at[d, chip], (tm, partner))
        for d in range(depth):
            for q in [partner] + [lax.rem(partner + 2 * i, ns) for i in range(1, others + 1)]:
                here = pfull.at[pl.ds(q * depth + d, 1)]
                remote(here, here, p_send.at[d, 0], p_recv.at[d, q], (tm, partner)).wait_recv()
        for copy in copies:
            copy.wait_send()

    @pl.when(tm < nt - 1)
    def _():
        for shift in shifts:
            shift.wait_send()

    arrive(4, mine=False)
    arrive(5)

    def save(j):
        for d in range(depth):
            put(relaxed.at[j], d, full[own + d])

    each_layer(lambda z: start_with(z, pfull[z]))
    phi(onward(5))
    save(0)
    for j in range(1, CF):
        phi(onward(1 + j))
        save(j)
    phi(to_full)
    for d in range(depth):
        qown[1, d] = full[own + d]
    back = remote(qown.at[1], qin, q_send, q_recv, (lax.rem(tm + 1, nt), s))

    @pl.when(tm < nt - 1)
    def _():
        back.start()

    @pl.when(tm == 0)
    def _():
        qin[...] = jnp.zeros(qin.shape, jnp.float32)

    @pl.when(tm > 0)
    def _():
        back.wait_recv()

    total = jnp.zeros((SUB, cols), jnp.float32)
    for d in range(depth):
        u0 = jnp.stack([relaxed[0, d, pl.ds(i, SUB, stride=lo), :] for i in range(lo)])
        r = natural(5, own + d) + qin[d] - u0
        put(resid.at[0], d, r)
        total = total + jnp.sum(r * r, axis=0)

    @pl.when(tm < nt - 1)
    def _():
        back.wait_send()

    parts[0] = total
    sends = []
    for i in range(1, ns):
        copy = remote(parts.at[0], allsp.at[s], n_send.at[0, i], n_recv.at[0, s],
                      (tm, lax.rem(s + i, ns)))
        copy.start()
        sends.append(copy)
    allsp[s] = total
    for i in range(1, ns):
        q = lax.rem(s + i, ns)
        remote(parts.at[0], allsp.at[q], n_send.at[0, i], n_recv.at[0, q], (tm, q)).wait_recv()
    total = allsp[0]
    for q in range(1, ns):
        total = total + allsp[q]
    parts[1] = total
    for i in range(1, nt):
        copy = remote(parts.at[1], alltm.at[tm], n_send.at[1, i], n_recv.at[1, tm],
                      (lax.rem(tm + i, nt), s))
        copy.start()
        sends.append(copy)
    alltm[tm] = total
    for i in range(1, nt):
        q = lax.rem(tm + i, nt)
        remote(parts.at[1], alltm.at[q], n_send.at[1, i], n_recv.at[1, q], (q, s)).wait_recv()
    total = alltm[0]
    for q in range(1, nt):
        total = total + alltm[q]
    norm[...] = jnp.full(norm.shape, jnp.sum(total), jnp.float32)
    for copy in sends + pending:
        copy.wait_send()


def local(nt, ns, state, source, absorption):
    depth, rows, cols = absorption.shape
    lo = rows // SUB
    layers = ns * depth
    others = ns // 2 - 1
    fields = CF + 2
    f32 = jnp.float32
    dma = pltpu.SemaphoreType.DMA
    big = max(ns, nt)
    relaxed, resid, norm = pl.pallas_call(
        functools.partial(kernel, nt, ns),
        out_shape=(
            jax.ShapeDtypeStruct(source.shape, f32),
            jax.ShapeDtypeStruct((1,) + absorption.shape, f32),
            jax.ShapeDtypeStruct((SUB, cols), f32),
        ),
        in_specs=[pl.BlockSpec(memory_space=pl.ANY)] * 3,
        out_specs=[pl.BlockSpec(memory_space=pltpu.VMEM)] * 3,
        scratch_shapes=[
            pltpu.VMEM((fields, layers, rows, cols), f32),
            pltpu.VMEM((layers, lo, SUB, cols), f32),
            pltpu.VMEM((layers + 2, lo, SUB, cols), f32),
            pltpu.VMEM((layers, lo, SUB, cols), f32),
            pltpu.VMEM((layers, lo, SUB, cols), f32),
            pltpu.VMEM((layers, lo, SUB, cols), f32),
            pltpu.VMEM((2, depth, lo, SUB, cols), f32),
            pltpu.VMEM((depth, lo, SUB, cols), f32),
            pltpu.VMEM((SUB, cols), f32),
            pltpu.VMEM((ns, SUB, cols), f32),
            pltpu.VMEM((nt, SUB, cols), f32),
            pltpu.VMEM((2, SUB, cols), f32),
            dma((fields,)),
            dma((fields, 1 + 2 * others)),
            dma((fields, ns)),
            dma((depth, 1 + 2 * others)),
            dma((depth, ns)),
            dma((depth,)),
            dma,
            dma,
            dma((2, big)),
            dma((2, big)),
        ],
        compiler_params=pltpu.CompilerParams(
            collective_id=0, has_side_effects=True, vmem_limit_bytes=48 * 1024 * 1024
        ),
        name="fcf",
    )(state, source, absorption)
    return relaxed, resid, norm[0, 0]


def solution(mesh):
    nt, ns = mesh.shape["tm"], mesh.shape["space"]
    return jax.shard_map(
        functools.partial(local, nt, ns),
        mesh=mesh,
        in_specs=(
            P("tm", "space", None, None),
            P("tm", "space", None, None),
            P("space", None, None),
        ),
        out_specs=(P("tm", "space", None, None), P("tm", "space", None, None), P()),
        check_vma=False,
    )
```

```python
import functools
import math

import jax
import jax.numpy as jnp
import numpy as np
from jax import lax
from jax.experimental import pallas as pl
from jax.experimental.pallas import tpu as pltpu
from jax.sharding import PartitionSpec as P

CF = 4
SWEEPS = 5
SUB = 8

coupling = 4.0
MESH = pl.DeviceIdType.MESH


def series():
    spread = 6.0 * coupling / (1.0 + 6.0 * coupling)
    one = np.polynomial.Polynomial([1.0])
    var = np.polynomial.Polynomial([0.0, 1.0])
    x = one
    for k in range(SWEEPS):
        weight = 1.0 / (1.0 + spread * math.cos(math.pi * (2 * k + 1) / (2 * SWEEPS)))
        x = x + weight * (one - (one - var) * x)
    c = x.coef
    return float(c[0]), float(c[2]), float(c[4])


def kernel(nt, ns, state, source, absorb, relaxed_out, resid_out, norm,
           relaxed, resid, nat, c4, work, held, full, pfull, qown, qin, tot, allsp, alltm, parts,
           loc_sem, g_send, g_recv, p_send, p_recv, sh_send, q_send, q_recv,
           n_send, n_recv, o_sem):
    tm = lax.axis_index("tm")
    s = lax.axis_index("space")
    depth, rows, cols = absorb.shape
    lo = rows // SUB
    layers = ns * depth
    others = ns // 2 - 1
    partner = s + 1 - 2 * lax.rem(s, 2)
    chips = [lax.rem(s + 2 * i, ns) for i in range(1, others + 1)]
    r0, r1, r2 = series()
    own = s * depth

    barrier = pltpu.get_barrier_semaphore()
    for i in range(1, ns):
        pl.semaphore_signal(barrier, inc=1, device_id=(tm, lax.rem(s + i, ns)), device_id_type=MESH)
    for i in range(1, nt):
        pl.semaphore_signal(barrier, inc=1, device_id=(lax.rem(tm + i, nt), s), device_id_type=MESH)

    srcs = [absorb, state.at[0]] + [source.at[j] for j in range(1, CF)] + [source.at[0]]
    fields = len(srcs)
    quarter = lambda f, q: nat.at[f, pl.ds(q * depth, depth)]
    loads = [pltpu.make_async_copy(srcs[f], quarter(f, s), loc_sem.at[f]) for f in range(fields)]
    for load in loads:
        load.start()
    work[0] = jnp.zeros(work.shape[1:], jnp.float32)
    work[layers + 1] = jnp.zeros(work.shape[1:], jnp.float32)

    pl.semaphore_wait(barrier, ns - 1 + nt - 1)

    def remote(src, dst, send, recv, where):
        return pltpu.make_async_remote_copy(
            src_ref=src, dst_ref=dst, send_sem=send, recv_sem=recv,
            device_id=where, device_id_type=MESH)

    pending = []

    def go(copy):
        copy.start()
        pending.append(copy)

    for f in range(fields):
        here = quarter(f, s)
        loads[f].wait()
        for i, chip in enumerate(chips):
            go(remote(here, here, g_send.at[f, 1 + i], g_recv.at[f, s], (tm, chip)))
        go(remote(here, here, g_send.at[f, 0], g_recv.at[f, s], (tm, partner)))

    def relay(f):
        for i, chip in enumerate(chips):
            here = quarter(f, chip)
            remote(here, here, g_send.at[f, 0], g_recv.at[f, chip], (tm, partner)).wait_recv()
            go(remote(here, here, g_send.at[f, 1 + others + i], g_recv.at[f, chip], (tm, partner)))

    def arrive(f):
        there = [partner] + [lax.rem(partner + 2 * i, ns) for i in range(1, others + 1)]
        for q in there:
            here = quarter(f, q)
            remote(here, here, g_send.at[f, 0], g_recv.at[f, q], (tm, partner)).wait_recv()

    def natural(f, z):
        return jnp.stack([nat[f, z, pl.ds(i, SUB, stride=lo), :] for i in range(lo)])

    lane = lax.broadcasted_iota(jnp.int32, (lo, SUB, cols), 2)
    first_lane, last_lane = lane == 0, lane == cols - 1
    sub = lax.broadcasted_iota(jnp.int32, (SUB, cols), 0)
    first_sub, last_sub = sub == 0, sub == SUB - 1

    def beside(v):
        up = jnp.where(first_sub, 0.0, pltpu.roll(v[lo - 1], 1, 0))
        down = jnp.where(last_sub, 0.0, pltpu.roll(v[0], SUB - 1, 0))
        total = jnp.concatenate([up[None], v[:-1]]) + jnp.concatenate([v[1:], down[None]])
        flat = v.reshape(lo * SUB, cols)
        left = pltpu.roll(flat, 1, 1).reshape(v.shape)
        right = pltpu.roll(flat, cols - 1, 1).reshape(v.shape)
        return total + jnp.where(first_lane, 0.0, left) + jnp.where(last_lane, 0.0, right)

    def sweep(finish, start=0, count=None):
        before, now = work[start], work[start + 1]
        for j in range(layers if count is None else count):
            z = start + j
            after = work[z + 2]
            finish(z, c4[z] * (before + after + beside(now)), now)
            before, now = now, after

    def plain(z, moved, now):
        work[z + 1] = moved

    def adding(factor):
        def finish(z, moved, now):
            work[z + 1] = moved + factor * held[z]
        return finish

    def start_with(z, value):
        h = value * (c4[z] * (r2 / coupling))
        work[z + 1] = h
        held[z] = h

    def phi(finish, mine=False):
        steps = [plain, adding(r1 / r2), plain, adding(r0 / r2), finish]
        for k, step in enumerate(steps):
            margin = len(steps) - 1 - k
            count = depth + 2 * margin
            if mine and count < layers:
                sweep(step, jnp.clip(own - margin, 0, layers - count), count)
            else:
                sweep(step)

    def each_layer(do):
        def body(z, _):
            do(z)
            return 0
        lax.fori_loop(0, layers, body, 0)

    def onward(f):
        def finish(z, moved, now):
            value = now + moved + natural(f, z)
            full[z] = value
            start_with(z, value)
        return finish

    def to_full(z, moved, now):
        full[z] = now + moved

    def put(ref, d, value):
        for i in range(lo):
            ref[d, pl.ds(i, SUB, stride=lo), :] = value[i]

    relay(0)
    relay(1)
    arrive(0)

    def scale(z):
        c4[z] = coupling / (1.0 + 6.0 * coupling + natural(0, z))
    each_layer(scale)
    relay(2)
    arrive(1)
    each_layer(lambda z: start_with(z, natural(1, z)))
    relay(3)
    arrive(2)
    phi(onward(2))
    relay(4)
    arrive(3)
    phi(onward(3))
    phi(to_full, mine=True)
    relay(5)

    chunk = lambda d: pl.ds(own + d, 1)
    for d in range(depth):
        qown[0, d] = full[own + d] + natural(4, own + d)
    shifts = [remote(qown.at[0, pl.ds(d, 1)], pfull.at[chunk(d)], sh_send.at[d], p_recv.at[d, s],
                     (lax.rem(tm + 1, nt), s)) for d in range(depth)]

    @pl.when(tm < nt - 1)
    def _():
        for shift in shifts:
            shift.start()

    @pl.when(tm == 0)
    def _():
        def zero(z):
            pfull[z] = jnp.zeros(pfull.shape[1:], jnp.float32)
        each_layer(zero)

    @pl.when(tm > 0)
    def _():
        copies = []

        def send(src, send_sem, recv_sem, where):
            copy = remote(src, src, send_sem, recv_sem, where)
            copy.start()
            copies.append(copy)

        for d in range(depth):
            here = pfull.at[chunk(d)]
            shifts[d].wait_recv()
            for i, chip in enumerate(chips):
                send(here, p_send.at[d, 1 + i], p_recv.at[d, s], (tm, chip))
            send(here, p_send.at[d, 0], p_recv.at[d, s], (tm, partner))
        for d in range(depth):
            for i, chip in enumerate(chips):
                here = pfull.at[pl.ds(chip * depth + d, 1)]
                remote(here, here, p_send.at[d, 0], p_recv.at[d, chip], (tm, partner)).wait_recv()
                send(here, p_send.at[d, 1 + others + i], p_recv.at[d, chip], (tm, partner))
        for d in range(depth):
            for q in [partner] + [lax.rem(partner + 2 * i, ns) for i in range(1, others + 1)]:
                here = pfull.at[pl.ds(q * depth + d, 1)]
                remote(here, here, p_send.at[d, 0], p_recv.at[d, q], (tm, partner)).wait_recv()
        for copy in copies:
            copy.wait_send()

    @pl.when(tm < nt - 1)
    def _():
        for shift in shifts:
            shift.wait_send()

    arrive(4)
    arrive(5)

    outs = []

    def save(j):
        for d in range(depth):
            put(relaxed.at[j], d, full[own + d])
        out = pltpu.make_async_copy(relaxed.at[j], relaxed_out.at[j], o_sem.at[j])
        out.start()
        outs.append(out)

    each_layer(lambda z: start_with(z, pfull[z]))
    phi(onward(5))
    save(0)
    for j in range(1, CF):
        phi(onward(1 + j))
        save(j)
    phi(to_full, mine=True)
    for d in range(depth):
        qown[1, d] = full[own + d]
    back = remote(qown.at[1], qin, q_send, q_recv, (lax.rem(tm + 1, nt), s))

    @pl.when(tm < nt - 1)
    def _():
        back.start()

    @pl.when(tm == 0)
    def _():
        qin[...] = jnp.zeros(qin.shape, jnp.float32)

    @pl.when(tm > 0)
    def _():
        back.wait_recv()

    total = jnp.zeros((SUB, cols), jnp.float32)
    for d in range(depth):
        u0 = jnp.stack([relaxed[0, d, pl.ds(i, SUB, stride=lo), :] for i in range(lo)])
        r = natural(5, own + d) + qin[d] - u0
        put(resid.at[0], d, r)
        total = total + jnp.sum(r * r, axis=0)

    @pl.when(tm < nt - 1)
    def _():
        back.wait_send()

    out = pltpu.make_async_copy(resid, resid_out, o_sem.at[CF])
    out.start()
    outs.append(out)
    parts[0] = total
    sends = []
    for i in range(1, ns):
        copy = remote(parts.at[0], allsp.at[s], n_send.at[0, i], n_recv.at[0, s],
                      (tm, lax.rem(s + i, ns)))
        copy.start()
        sends.append(copy)
    allsp[s] = total
    for i in range(1, ns):
        q = lax.rem(s + i, ns)
        remote(parts.at[0], allsp.at[q], n_send.at[0, i], n_recv.at[0, q], (tm, q)).wait_recv()
    total = allsp[0]
    for q in range(1, ns):
        total = total + allsp[q]
    parts[1] = total
    for i in range(1, nt):
        copy = remote(parts.at[1], alltm.at[tm], n_send.at[1, i], n_recv.at[1, tm],
                      (lax.rem(tm + i, nt), s))
        copy.start()
        sends.append(copy)
    alltm[tm] = total
    for i in range(1, nt):
        q = lax.rem(tm + i, nt)
        remote(parts.at[1], alltm.at[q], n_send.at[1, i], n_recv.at[1, q], (q, s)).wait_recv()
    total = alltm[0]
    for q in range(1, nt):
        total = total + alltm[q]
    norm[0] = jnp.sum(total)
    for copy in sends + pending:
        copy.wait_send()
    for out in outs:
        out.wait()


def local(nt, ns, state, source, absorption):
    depth, rows, cols = absorption.shape
    lo = rows // SUB
    layers = ns * depth
    others = ns // 2 - 1
    fields = CF + 2
    f32 = jnp.float32
    dma = pltpu.SemaphoreType.DMA
    big = max(ns, nt)
    relaxed, resid, norm = pl.pallas_call(
        functools.partial(kernel, nt, ns),
        out_shape=(
            jax.ShapeDtypeStruct(source.shape, f32),
            jax.ShapeDtypeStruct((1,) + absorption.shape, f32),
            jax.ShapeDtypeStruct((1,), f32),
        ),
        in_specs=[pl.BlockSpec(memory_space=pltpu.HBM)] * 3,
        out_specs=[pl.BlockSpec(memory_space=pltpu.HBM)] * 2
        + [pl.BlockSpec(memory_space=pltpu.SMEM)],
        scratch_shapes=[
            pltpu.VMEM(source.shape, f32),
            pltpu.VMEM((1,) + absorption.shape, f32),
            pltpu.VMEM((fields, layers, rows, cols), f32),
            pltpu.VMEM((layers, lo, SUB, cols), f32),
            pltpu.VMEM((layers + 2, lo, SUB, cols), f32),
            pltpu.VMEM((layers, lo, SUB, cols), f32),
            pltpu.VMEM((layers, lo, SUB, cols), f32),
            pltpu.VMEM((layers, lo, SUB, cols), f32),
            pltpu.VMEM((2, depth, lo, SUB, cols), f32),
            pltpu.VMEM((depth, lo, SUB, cols), f32),
            pltpu.VMEM((SUB, cols), f32),
            pltpu.VMEM((ns, SUB, cols), f32),
            pltpu.VMEM((nt, SUB, cols), f32),
            pltpu.VMEM((2, SUB, cols), f32),
            dma((fields,)),
            dma((fields, 1 + 2 * others)),
            dma((fields, ns)),
            dma((depth, 1 + 2 * others)),
            dma((depth, ns)),
            dma((depth,)),
            dma,
            dma,
            dma((2, big)),
            dma((2, big)),
            dma((CF + 1,)),
        ],
        compiler_params=pltpu.CompilerParams(
            collective_id=0, has_side_effects=True, vmem_limit_bytes=60 * 1024 * 1024
        ),
        name="fcf",
    )(state, source, absorption)
    return relaxed, resid, norm.reshape(())


def solution(mesh):
    nt, ns = mesh.shape["tm"], mesh.shape["space"]
    return jax.shard_map(
        functools.partial(local, nt, ns),
        mesh=mesh,
        in_specs=(
            P("tm", "space", None, None),
            P("tm", "space", None, None),
            P("space", None, None),
        ),
        out_specs=(P("tm", "space", None, None), P("tm", "space", None, None), P()),
        check_vma=False,
    )
```

```python
import functools
import math

import jax
import jax.numpy as jnp
import numpy as np
from jax import lax
from jax.experimental import pallas as pl
from jax.experimental.pallas import tpu as pltpu
from jax.sharding import PartitionSpec as P

CF = 4
SWEEPS = 5
SUB = 8

coupling = 4.0
MESH = pl.DeviceIdType.MESH


def series():
    spread = 6.0 * coupling / (1.0 + 6.0 * coupling)
    one = np.polynomial.Polynomial([1.0])
    var = np.polynomial.Polynomial([0.0, 1.0])
    x = one
    for k in range(SWEEPS):
        weight = 1.0 / (1.0 + spread * math.cos(math.pi * (2 * k + 1) / (2 * SWEEPS)))
        x = x + weight * (one - (one - var) * x)
    c = x.coef
    return float(c[0]), float(c[2]), float(c[4])


def kernel(nt, ns, state, source, absorb, relaxed_out, resid_out, norm,
           relaxed, resid, nat, c4, work, held, full, pfull, qown, qin, eown, ein, tot, allsp, alltm, parts,
           loc_sem, g_send, g_recv, p_send, p_recv, sh_send, q_send, q_recv, e_send, e_recv,
           n_send, n_recv, o_sem):
    tm = lax.axis_index("tm")
    s = lax.axis_index("space")
    depth, rows, cols = absorb.shape
    lo = rows // SUB
    layers = ns * depth
    others = ns // 2 - 1
    partner = s + 1 - 2 * lax.rem(s, 2)
    chips = [lax.rem(s + 2 * i, ns) for i in range(1, others + 1)]
    r0, r1, r2 = series()
    own = s * depth

    barrier = pltpu.get_barrier_semaphore()
    for i in range(1, ns):
        pl.semaphore_signal(barrier, inc=1, device_id=(tm, lax.rem(s + i, ns)), device_id_type=MESH)
    for i in range(1, nt):
        pl.semaphore_signal(barrier, inc=1, device_id=(lax.rem(tm + i, nt), s), device_id_type=MESH)

    srcs = [absorb, state.at[0]] + [source.at[j] for j in range(1, CF)] + [source.at[0]]
    fields = len(srcs)
    quarter = lambda f, q: nat.at[f, pl.ds(q * depth, depth)]
    loads = [pltpu.make_async_copy(srcs[f], quarter(f, s), loc_sem.at[f]) for f in range(fields)]
    for load in loads:
        load.start()
    work[0] = jnp.zeros(work.shape[1:], jnp.float32)
    work[layers + 1] = jnp.zeros(work.shape[1:], jnp.float32)

    pl.semaphore_wait(barrier, ns - 1 + nt - 1)

    def remote(src, dst, send, recv, where):
        return pltpu.make_async_remote_copy(
            src_ref=src, dst_ref=dst, send_sem=send, recv_sem=recv,
            device_id=where, device_id_type=MESH)

    pending = []
    late = CF

    def go(copy):
        copy.start()
        pending.append(copy)

    def spread(f):
        here = quarter(f, s)
        if f != late:
            loads[f].wait()
        for i, chip in enumerate(chips):
            go(remote(here, here, g_send.at[f, 1 + i], g_recv.at[f, s], (tm, chip)))
        go(remote(here, here, g_send.at[f, 0], g_recv.at[f, s], (tm, partner)))

    for f in range(fields):
        if f != late:
            spread(f)

    def relay(f):
        for i, chip in enumerate(chips):
            here = quarter(f, chip)
            remote(here, here, g_send.at[f, 0], g_recv.at[f, chip], (tm, partner)).wait_recv()
            go(remote(here, here, g_send.at[f, 1 + others + i], g_recv.at[f, chip], (tm, partner)))

    def arrive(f):
        there = [partner] + [lax.rem(partner + 2 * i, ns) for i in range(1, others + 1)]
        for q in there:
            here = quarter(f, q)
            remote(here, here, g_send.at[f, 0], g_recv.at[f, q], (tm, partner)).wait_recv()

    def natural(f, z):
        return jnp.stack([nat[f, z, pl.ds(i, SUB, stride=lo), :] for i in range(lo)])

    lane = lax.broadcasted_iota(jnp.int32, (lo, SUB, cols), 2)
    first_lane, last_lane = lane == 0, lane == cols - 1
    sub = lax.broadcasted_iota(jnp.int32, (SUB, cols), 0)
    first_sub, last_sub = sub == 0, sub == SUB - 1

    def beside(v):
        up = jnp.where(first_sub, 0.0, pltpu.roll(v[lo - 1], 1, 0))
        down = jnp.where(last_sub, 0.0, pltpu.roll(v[0], SUB - 1, 0))
        total = jnp.concatenate([up[None], v[:-1]]) + jnp.concatenate([v[1:], down[None]])
        flat = v.reshape(lo * SUB, cols)
        left = pltpu.roll(flat, 1, 1).reshape(v.shape)
        right = pltpu.roll(flat, cols - 1, 1).reshape(v.shape)
        return total + jnp.where(first_lane, 0.0, left) + jnp.where(last_lane, 0.0, right)

    def sweep(finish, start=0, count=None):
        before, now = work[start], work[start + 1]
        for j in range(layers if count is None else count):
            z = start + j
            after = work[z + 2]
            finish(z, c4[z] * (before + after + beside(now)), now)
            before, now = now, after

    def plain(z, moved, now):
        work[z + 1] = moved

    def adding(factor):
        def finish(z, moved, now):
            work[z + 1] = moved + factor * held[z]
        return finish

    def start_with(z, value):
        h = value * (c4[z] * (r2 / coupling))
        work[z + 1] = h
        held[z] = h

    def phi(finish, mine=False):
        steps = [plain, adding(r1 / r2), plain, adding(r0 / r2), finish]
        for k, step in enumerate(steps):
            margin = len(steps) - 1 - k
            count = depth + 2 * margin
            if mine and count < layers:
                sweep(step, jnp.clip(own - margin, 0, layers - count), count)
            else:
                sweep(step)

    def each_layer(do):
        def body(z, _):
            do(z)
            return 0
        lax.fori_loop(0, layers, body, 0)

    def onward(f):
        def finish(z, moved, now):
            value = now + moved + natural(f, z)
            full[z] = value
            start_with(z, value)
        return finish

    def to_full(z, moved, now):
        full[z] = now + moved

    def put(ref, d, value):
        for i in range(lo):
            ref[d, pl.ds(i, SUB, stride=lo), :] = value[i]

    relay(0)
    relay(1)
    arrive(0)

    def scale(z):
        c4[z] = coupling / (1.0 + 6.0 * coupling + natural(0, z))
    each_layer(scale)
    relay(2)
    arrive(1)
    each_layer(lambda z: start_with(z, natural(1, z)))
    relay(3)
    arrive(2)
    phi(onward(2))
    arrive(3)
    phi(onward(3))
    phi(to_full, mine=True)
    relay(5)

    loads[late].wait()

    chunk = lambda d: pl.ds(own + d, 1)
    for d in range(depth):
        qown[0, d] = full[own + d] + natural(late, own + d)
    shifts = [remote(qown.at[0, pl.ds(d, 1)], pfull.at[chunk(d)], sh_send.at[d], p_recv.at[d, s],
                     (lax.rem(tm + 1, nt), s)) for d in range(depth)]

    @pl.when(tm < nt - 1)
    def _():
        for shift in shifts:
            shift.start()

    @pl.when(tm == 0)
    def _():
        def zero(z):
            pfull[z] = jnp.zeros(pfull.shape[1:], jnp.float32)
        each_layer(zero)

    @pl.when(tm > 0)
    def _():
        copies = []

        def send(src, send_sem, recv_sem, where):
            copy = remote(src, src, send_sem, recv_sem, where)
            copy.start()
            copies.append(copy)

        for d in range(depth):
            here = pfull.at[chunk(d)]
            shifts[d].wait_recv()
            for i, chip in enumerate(chips):
                send(here, p_send.at[d, 1 + i], p_recv.at[d, s], (tm, chip))
            send(here, p_send.at[d, 0], p_recv.at[d, s], (tm, partner))
        for d in range(depth):
            for i, chip in enumerate(chips):
                here = pfull.at[pl.ds(chip * depth + d, 1)]
                remote(here, here, p_send.at[d, 0], p_recv.at[d, chip], (tm, partner)).wait_recv()
                send(here, p_send.at[d, 1 + others + i], p_recv.at[d, chip], (tm, partner))
        for d in range(depth):
            for q in [partner] + [lax.rem(partner + 2 * i, ns) for i in range(1, others + 1)]:
                here = pfull.at[pl.ds(q * depth + d, 1)]
                remote(here, here, p_send.at[d, 0], p_recv.at[d, q], (tm, partner)).wait_recv()
        for copy in copies:
            copy.wait_send()

    @pl.when(tm < nt - 1)
    def _():
        for shift in shifts:
            shift.wait_send()

    spread(late)
    arrive(5)

    outs = []

    def save(j):
        for d in range(depth):
            put(relaxed.at[j], d, full[own + d])
        out = pltpu.make_async_copy(relaxed.at[j], relaxed_out.at[j], o_sem.at[j])
        out.start()
        outs.append(out)

    each_layer(lambda z: start_with(z, pfull[z]))
    phi(onward(5))
    save(0)
    for d in range(depth):
        eown[d] = natural(5, own + d) - full[own + d]
    rest = remote(eown, ein, e_send, e_recv, (lax.rem(tm + nt - 1, nt), s))

    @pl.when(tm > 0)
    def _():
        rest.start()

    for j in range(1, CF):
        if 1 + j == late:
            relay(late)
            arrive(late)
        phi(onward(1 + j))
        save(j)
    phi(to_full, mine=True)
    for d in range(depth):
        qown[1, d] = full[own + d]
    back = remote(qown.at[1], qin, q_send, q_recv, (lax.rem(tm + 1, nt), s))

    @pl.when(tm < nt - 1)
    def _():
        back.start()

    def squares(value):
        return jnp.sum(value * value, axis=(0, 1))

    tot[...] = jnp.zeros(tot.shape, jnp.float32)

    @pl.when(tm == 0)
    def _():
        qin[...] = jnp.zeros(qin.shape, jnp.float32)
        tot[...] = squares(eown[...])

    @pl.when(tm < nt - 1)
    def _():
        rest.wait_recv()
        tot[...] = tot[...] + squares(qown[1] + ein[...])

    total = tot[...]
    parts[0] = total
    sends = []
    for i in range(1, ns):
        copy = remote(parts.at[0], allsp.at[s], n_send.at[0, i], n_recv.at[0, s],
                      (tm, lax.rem(s + i, ns)))
        copy.start()
        sends.append(copy)
    allsp[s] = total
    for i in range(1, ns):
        q = lax.rem(s + i, ns)
        remote(parts.at[0], allsp.at[q], n_send.at[0, i], n_recv.at[0, q], (tm, q)).wait_recv()
    total = allsp[0]
    for q in range(1, ns):
        total = total + allsp[q]
    parts[1] = total
    for i in range(1, nt):
        copy = remote(parts.at[1], alltm.at[tm], n_send.at[1, i], n_recv.at[1, tm],
                      (lax.rem(tm + i, nt), s))
        copy.start()
        sends.append(copy)
    alltm[tm] = total
    for i in range(1, nt):
        q = lax.rem(tm + i, nt)
        remote(parts.at[1], alltm.at[q], n_send.at[1, i], n_recv.at[1, q], (q, s)).wait_recv()
    total = alltm[0]
    for q in range(1, nt):
        total = total + alltm[q]
    norm[0] = jnp.sum(total)

    @pl.when(tm > 0)
    def _():
        back.wait_recv()

    for d in range(depth):
        put(resid.at[0], d, qin[d] + eown[d])
    out = pltpu.make_async_copy(resid, resid_out, o_sem.at[CF])
    out.start()
    outs.append(out)

    @pl.when(tm < nt - 1)
    def _():
        back.wait_send()

    @pl.when(tm > 0)
    def _():
        rest.wait_send()

    for copy in sends + pending:
        copy.wait_send()
    for out in outs:
        out.wait()


def local(nt, ns, state, source, absorption):
    depth, rows, cols = absorption.shape
    lo = rows // SUB
    layers = ns * depth
    others = ns // 2 - 1
    fields = CF + 2
    f32 = jnp.float32
    dma = pltpu.SemaphoreType.DMA
    big = max(ns, nt)
    relaxed, resid, norm = pl.pallas_call(
        functools.partial(kernel, nt, ns),
        out_shape=(
            jax.ShapeDtypeStruct(source.shape, f32),
            jax.ShapeDtypeStruct((1,) + absorption.shape, f32),
            jax.ShapeDtypeStruct((1,), f32),
        ),
        in_specs=[pl.BlockSpec(memory_space=pltpu.HBM)] * 3,
        out_specs=[pl.BlockSpec(memory_space=pltpu.HBM)] * 2
        + [pl.BlockSpec(memory_space=pltpu.SMEM)],
        scratch_shapes=[
            pltpu.VMEM(source.shape, f32),
            pltpu.VMEM((1,) + absorption.shape, f32),
            pltpu.VMEM((fields, layers, rows, cols), f32),
            pltpu.VMEM((layers, lo, SUB, cols), f32),
            pltpu.VMEM((layers + 2, lo, SUB, cols), f32),
            pltpu.VMEM((layers, lo, SUB, cols), f32),
            pltpu.VMEM((layers, lo, SUB, cols), f32),
            pltpu.VMEM((layers, lo, SUB, cols), f32),
            pltpu.VMEM((2, depth, lo, SUB, cols), f32),
            pltpu.VMEM((depth, lo, SUB, cols), f32),
            pltpu.VMEM((depth, lo, SUB, cols), f32),
            pltpu.VMEM((depth, lo, SUB, cols), f32),
            pltpu.VMEM((SUB, cols), f32),
            pltpu.VMEM((ns, SUB, cols), f32),
            pltpu.VMEM((nt, SUB, cols), f32),
            pltpu.VMEM((2, SUB, cols), f32),
            dma((fields,)),
            dma((fields, 1 + 2 * others)),
            dma((fields, ns)),
            dma((depth, 1 + 2 * others)),
            dma((depth, ns)),
            dma((depth,)),
            dma,
            dma,
            dma,
            dma,
            dma((2, big)),
            dma((2, big)),
            dma((CF + 1,)),
        ],
        compiler_params=pltpu.CompilerParams(
            collective_id=0, has_side_effects=True, vmem_limit_bytes=60 * 1024 * 1024
        ),
        name="fcf",
    )(state, source, absorption)
    return relaxed, resid, norm.reshape(())


def solution(mesh):
    nt, ns = mesh.shape["tm"], mesh.shape["space"]
    return jax.shard_map(
        functools.partial(local, nt, ns),
        mesh=mesh,
        in_specs=(
            P("tm", "space", None, None),
            P("tm", "space", None, None),
            P("space", None, None),
        ),
        out_specs=(P("tm", "space", None, None), P("tm", "space", None, None), P()),
        check_vma=False,
    )
```
